32 devices in a mesh: pulse: 4 (over y, x), tile: 8 (over z, core).
Axes of the slice: x: 2, y: 2, z: 4, core: 2. Of those that a mesh axis runs over, the one named last changes fastest.
Arguments:
- pulses: bfloat16 [4096, 2, 4096], P(None, None, ('pulse', 'tile')), may hold values from -6 to 6
- steering: bfloat16 [2, 128, 128], replicated, may hold values from -0.375 to 0.375
- merge_re: bfloat16 [3, 256, 256], replicated, may hold values from -0.25 to 0.25
- merge_im: bfloat16 [3, 256, 256], replicated, may hold values from -0.25 to 0.25
- range_shift: int32 [3, 2, 128], replicated, may hold values from -8 to 8
- image_map: bfloat16 [4, 8, 2, 128, 512], P('pulse', 'tile'), may hold values from -0.0625 to 0.0625
Outputs:
- image: float32 [4096, 1024], P(('pulse', 'tile'))
The draws below stay inside these ranges and needn't reach their ends.
All inputs are finite; a program needn't handle non-finite values.
Results may differ from the reference program's by a relative error of at most 0.0057.
Values may be sent and summed in bfloat16 or wider, within the bound.
A program may use at most 64 MiB of HBM per device.

```python
import jax
import jax.numpy as jnp
import numpy as np
from jax import lax

R = 4096
PD = 128
K = 128
X = 512
LEVELS = 3
SHIFT = 8
GROUPS = 4
SUBS = 8
N_PULSE = 4
N_TILE = 8
DEVICES = 32


def place_ends(array, own_key, low, largest):
    place = [jax.random.randint(jax.random.fold_in(own_key, axis), (), 0, length) for axis, length in enumerate(array.shape)]
    main_axis = array.shape.index(max(array.shape))
    neighbour = place[:main_axis] + [(place[main_axis] + 1) % array.shape[main_axis]] + place[main_axis + 1:]
    return array.at[tuple(place)].set(low).at[tuple(neighbour)].set(largest)


def levels(rng, shape, split, least, high):
    loudness, own = 1.0, jax.random.fold_in(rng, 6)
    for axis_at, blocks in split:
        steps = jnp.exp(jax.random.uniform(jax.random.fold_in(own, axis_at), (blocks,), jnp.float32, least / len(split), high / len(split)))
        loudness = loudness * jnp.repeat(steps, shape[axis_at] // blocks).reshape([-1 if axis == axis_at else 1 for axis in range(len(shape))])
    return loudness


def scatter_about(stream_key, shape, spread, limit, cuts=(), kind=jnp.bfloat16):
    entries = jax.random.normal(stream_key, shape, jnp.float32) * spread
    if len(cuts) > 0:
        entries = levels(stream_key, shape, cuts, -0.22, 0.18) * entries
    return jnp.clip(entries, min=-limit, max=limit).astype(kind)


def setup_inputs(seed: int = 0) -> dict:
    key_list = jax.random.split(jax.random.key(seed), 7)
    pulses = scatter_about(key_list[0], (R, 2, PD * DEVICES), 1.0, 6.0, ((2, 32),))
    steering = scatter_about(key_list[1], (2, PD, K), (2 * PD) ** -0.5, 0.375)
    merge_re = scatter_about(key_list[2], (LEVELS, 2 * K, 2 * K), (4 * K) ** -0.5, 0.25)
    merge_im = scatter_about(key_list[3], (LEVELS, 2 * K, 2 * K), (4 * K) ** -0.5, 0.25)
    range_shift = place_ends(jax.random.randint(key_list[4], (LEVELS, 2, K), 0 - SHIFT, SHIFT + 1), jax.random.fold_in(key_list[4], 1), 0 - SHIFT, SHIFT).astype(jnp.int32)
    image_map = scatter_about(key_list[5], (GROUPS, SUBS, 2, K, X), (2 * K * DEVICES) ** -0.5, 0.0625, ((0, 4), (1, 8)))
    return {"pulses": pulses, "steering": steering, "merge_re": merge_re, "merge_im": merge_im, "range_shift": range_shift, "image_map": image_map}


def complex_block(real_part, imag_part):
    upper_half = jnp.concatenate([real_part, imag_part], axis=1)
    lower_half = jnp.concatenate([-imag_part, real_part], axis=1)
    return jnp.concatenate([upper_half, lower_half], axis=0)


def shift_rows(beam_rows, shift_table):
    range_rows = beam_rows.shape[0]
    doubled = jnp.concatenate([shift_table, shift_table]).astype(jnp.int32)
    source = jnp.arange(range_rows, dtype=jnp.int32)[:, None] + doubled[None, :]
    inside = (source >= 0) & (source < range_rows)
    picked = jnp.take_along_axis(beam_rows, jnp.clip(source, 0, range_rows - 1), axis=0)
    return jnp.where(inside, picked, jnp.zeros_like(picked))


def reference(pulses, steering, merge_re, merge_im, range_shift, image_map):
    steer_block = complex_block(steering[0], steering[1]).astype(jnp.float32)
    shaped = pulses.reshape(R, 2, N_PULSE, N_TILE, PD).transpose(2, 3, 0, 1, 4).reshape(N_PULSE, N_TILE, R, 2 * PD)
    level_blocks = []
    for merge_level in range(LEVELS):
        chosen = []
        for half_bit in range(2):
            weight_re = merge_re[merge_level][:, half_bit * K:(half_bit + 1) * K]
            weight_im = merge_im[merge_level][:, half_bit * K:(half_bit + 1) * K]
            chosen.append(complex_block(weight_re, weight_im))
        level_blocks.append(jnp.stack(chosen))

    def group_term(running_sum, inputs):
        pulse_block, group_maps = inputs
        current = jnp.einsum("srp,pk->srk", pulse_block.astype(jnp.float32), steer_block).astype(jnp.bfloat16)
        for merge_level in range(LEVELS):
            partner_index = np.arange(N_TILE) ^ (1 << merge_level)
            halves = (np.arange(N_TILE) >> merge_level) & 1
            partner = current[partner_index]
            is_upper = jnp.asarray(halves == 1)[:, None, None]
            lower_src = jnp.where(is_upper, partner, current)
            upper_src = jnp.where(is_upper, current, partner)
            shifted_lower = jax.vmap(shift_rows, (0, None))(lower_src, range_shift[merge_level, 0])
            shifted_upper = jax.vmap(shift_rows, (0, None))(upper_src, range_shift[merge_level, 1])
            combined = jnp.concatenate([shifted_lower[..., :K], shifted_upper[..., :K], shifted_lower[..., K:], shifted_upper[..., K:]], axis=-1)
            per_sub = level_blocks[merge_level][halves]
            current = jnp.einsum("srk,skn->srn", combined.astype(jnp.float32), per_sub.astype(jnp.float32)).astype(jnp.bfloat16)
        map_blocks = jax.vmap(complex_block)(group_maps[:, 0], group_maps[:, 1])
        contribution = jnp.einsum("srk,skx->rx", current.astype(jnp.float32), map_blocks.astype(jnp.float32))
        return running_sum + contribution, None

    start_sum = jnp.zeros((R, 2 * X), jnp.float32)
    image, _ = lax.scan(group_term, start_sum, (shaped, image_map))
    return image
```

```python
import functools

import jax
import jax.numpy as jnp
from jax import lax
from jax.experimental import pallas as pl
from jax.experimental.pallas import tpu as pltpu
from jax.sharding import PartitionSpec as P

SHIFT = 8
PAD = 16
MESH = pl.DeviceIdType.MESH
F32 = jnp.float32
BF16 = jnp.bfloat16


def bit_of(index, place):
    return index // 2**place % 2


def flip(index, place):
    return index + (1 - 2 * bit_of(index, place)) * 2**place


def complex_block(real_part, imag_part):
    upper_half = jnp.concatenate([real_part, imag_part], axis=1)
    lower_half = jnp.concatenate([-imag_part, real_part], axis=1)
    return jnp.concatenate([upper_half, lower_half], axis=0)


def orders(pulse_bits, tile_bits):
    pulse = [("pulse", place) for place in range(pulse_bits)]
    tile = [("tile", place) for place in range(1, tile_bits)]
    return [pulse + tile, pulse[::-1] + tile]


def shifted(ref, start, rows, table):
    piece = ref[pl.ds(start, rows + 2 * PAD), :].astype(F32)[PAD - SHIFT :]
    held = piece.shape[0]
    for step in (1, 2, 4):
        piece = jnp.where((table & step) != 0, pltpu.roll(piece, held - step, 0), piece)
    piece = jnp.where((table & 8) != 0, piece[8 : rows + 24], piece[: rows + 16])
    return jnp.where((table & 16) != 0, piece[16 : rows + 16], piece[:rows]).astype(BF16)


def kernel(
    pulse_bits, tile_bits, block_rows, width,
    rows_ref, steer_ref, w0_ref, w1_ref, w2_ref, map_ref, table_ref, out_ref,
    b0, bp, b1, b2, b3, map_in, own, other, final, acc, send, recv,
    beam_s, beam_r, map_s, map_r, n_s, n_r, sum_s, sum_r,
):
    p, t = lax.axis_index("pulse"), lax.axis_index("tile")
    where = {"pulse": p, "tile": t}
    total = rows_ref.shape[0]
    beams = map_ref.shape[1]
    columns = map_ref.shape[2]
    chunks = 2 * columns // width
    streams = orders(pulse_bits, tile_bits)
    steps = pulse_bits + tile_bits
    tile = 512

    def device(axis, place):
        found = dict(where)
        found[axis] = flip(where[axis], place)
        return (found["pulse"], found["tile"])

    partners = [("pulse", place) for place in range(pulse_bits)]
    partners += [("tile", place) for place in range(tile_bits)]
    barrier = pltpu.get_barrier_semaphore()
    for axis, place in partners:
        pl.semaphore_signal(barrier, inc=1, device_id=device(axis, place), device_id_type=MESH)
    for ref in (b0, bp, b1, b2):
        edge = jnp.zeros((PAD, ref.shape[1]), BF16)
        ref[0:PAD, :] = edge
        ref[PAD + total : 2 * PAD + total, :] = edge
    pl.semaphore_wait(barrier, len(partners))

    map_copy = pltpu.make_async_remote_copy(
        src_ref=map_ref, dst_ref=map_in, send_sem=map_s, recv_sem=map_r,
        device_id=device("tile", 2), device_id_type=MESH,
    )
    map_copy.start()

    parts = 4
    part = total // parts
    beam_copies = []
    for piece in range(parts):

        @pl.loop(0, part // tile)
        def _(i, piece=piece):
            start = pl.multiple_of(piece * part + i * tile, tile)
            b0[pl.ds(start + PAD, tile), :] = jnp.dot(
                rows_ref[pl.ds(start, tile), :], steer_ref[...], preferred_element_type=F32
            ).astype(BF16)

        span = pl.ds(PAD + piece * part, part)
        copy = pltpu.make_async_remote_copy(
            src_ref=b0.at[span, :], dst_ref=bp.at[span, :],
            send_sem=beam_s.at[piece], recv_sem=beam_r.at[piece],
            device_id=device("tile", 0), device_id_type=MESH,
        )
        copy.start()
        beam_copies.append(copy)
    for copy in beam_copies:
        copy.wait_recv()

    @pl.loop(0, total // tile)
    def _(i):
        start = pl.multiple_of(i * tile, tile)
        mine = shifted(b0, start, tile, table_ref[0:1, : 2 * beams])
        theirs = shifted(bp, start, tile, table_ref[1:2, : 2 * beams])
        merged = jnp.dot(mine, w0_ref[: 2 * beams, :], preferred_element_type=F32)
        merged += jnp.dot(theirs, w0_ref[2 * beams :, :], preferred_element_type=F32)
        b1[pl.ds(start + PAD, tile), :] = merged.astype(BF16)

    map_copy.wait_recv()
    weights = [w2_ref[i] for i in range(4)]

    def product(left, right):
        return jnp.dot(left, right, preferred_element_type=F32)

    own[0] = (
        product(weights[0], map_ref[0]) - product(weights[1], map_ref[1])
        + product(weights[2], map_in[0]) - product(weights[3], map_in[1])
    ).astype(BF16)
    own[1] = (
        product(weights[0], map_ref[1]) + product(weights[1], map_ref[0])
        + product(weights[2], map_in[1]) + product(weights[3], map_in[0])
    ).astype(BF16)
    n_copy = pltpu.make_async_remote_copy(
        src_ref=own, dst_ref=other, send_sem=n_s, recv_sem=n_r,
        device_id=device("tile", 1), device_id_type=MESH,
    )
    n_copy.start()

    @pl.loop(0, total // tile)
    def _(i):
        start = pl.multiple_of(i * tile, tile)
        mine = shifted(b1, start, tile, table_ref[2:3, : 2 * beams])
        b2[pl.ds(start + PAD, tile), :] = jnp.dot(
            mine, w1_ref[...], preferred_element_type=F32
        ).astype(BF16)

    @pl.loop(0, total // tile)
    def _(i):
        start = pl.multiple_of(i * tile, tile)
        b3[pl.ds(start, tile), :] = shifted(b2, start, tile, table_ref[3:4, :])

    n_copy.wait_recv()
    for at, source in ((0, own), (2 * beams, other)):
        final[at : at + beams, :columns] = source[0]
        final[at : at + beams, columns:] = source[1]
        final[at + beams : at + 2 * beams, :columns] = -source[1]
        final[at + beams : at + 2 * beams, columns:] = source[0]

    core = bit_of(t, 0)
    half = total // 2
    bases = [total - (total >> step) for step in range(steps)]
    copies = {}

    def launch(step, chunk, axis, place):
        span = pl.ds(bases[step], half >> step)
        copies[step, chunk] = copy = pltpu.make_async_remote_copy(
            src_ref=send.at[chunk, span, :], dst_ref=recv.at[chunk, span, :],
            send_sem=sum_s.at[step, chunk], recv_sem=sum_r.at[step, chunk],
            device_id=device(axis, place), device_id_type=MESH,
        )
        copy.start()

    def form(chunk_set):
        first = chunk_set[0] * width
        last = first + len(chunk_set) * width

        @pl.loop(0, total // tile)
        def _(i):
            start = pl.multiple_of(i * tile, tile)
            value = jnp.dot(
                b3[pl.ds(start, tile), :], final[:, first:last], preferred_element_type=F32
            )
            for pair in range(tile // (2 * block_rows)):
                low = value[2 * pair * block_rows : (2 * pair + 1) * block_rows]
                high = value[(2 * pair + 1) * block_rows : (2 * pair + 2) * block_rows]
                keep = jnp.where(core == 0, low, high)
                leave = jnp.where(core == 0, high, low).astype(BF16)
                number = i * (tile // (2 * block_rows)) + pair
                for at, chunk in enumerate(chunk_set):
                    order = streams[chunk % len(streams)]
                    index = 0
                    for axis, place in order:
                        where_bit = place - 1 if axis == "tile" else place + tile_bits - 1
                        index = index * 2 + bit_of(number, where_bit)
                    span = pl.ds(pl.multiple_of(index * block_rows, block_rows), block_rows)
                    acc[chunk, span, :] = keep[:, at * width : (at + 1) * width]
                    send[chunk, span, :] = leave[:, at * width : (at + 1) * width]

        for chunk in chunk_set:
            launch(0, chunk, "tile", 0)

    bases_live = {chunk: 0 for chunk in range(chunks)}

    def fold(step, chunk):
        copies[step, chunk].wait_recv()
        rows = half >> step
        live = bases_live[chunk]
        if step == steps - 1:
            span = pl.ds(pl.multiple_of(live, rows), rows)
            got = recv[chunk, pl.ds(bases[step], rows), :].astype(F32)
            out_ref[:, chunk * width : (chunk + 1) * width] = acc[chunk, span, :] + got
            return
        axis, place = streams[chunk % len(streams)][step]
        rest = rows // 2
        kept = bit_of(where[axis], place)
        size = min(rest, 256)

        @pl.loop(0, rest // size)
        def _(i):
            at = (1 - kept) * rest + i * size
            value = acc[chunk, pl.ds(pl.multiple_of(live + at, size), size), :]
            value += recv[chunk, pl.ds(pl.multiple_of(bases[step] + at, size), size), :].astype(F32)
            to = pl.ds(pl.multiple_of(bases[step + 1] + i * size, size), size)
            send[chunk, to, :] = value.astype(BF16)

        launch(step + 1, chunk, axis, place)

        @pl.loop(0, rest // size)
        def _(i):
            at = kept * rest + i * size
            span = pl.ds(pl.multiple_of(live + at, size), size)
            got = recv[chunk, pl.ds(pl.multiple_of(bases[step] + at, size), size), :]
            acc[chunk, span, :] += got.astype(F32)

        bases_live[chunk] = live + kept * rest

    sets = [[2 * i, 2 * i + 1] for i in range(chunks // 2)]
    for i, chunk_set in enumerate(sets):
        form(chunk_set)
        if i > 0:
            for chunk in sets[i - 1]:
                fold(0, chunk)
    for chunk in sets[-1]:
        fold(0, chunk)
    for step in range(1, steps):
        for chunk in range(chunks):
            fold(step, chunk)

    map_copy.wait_send()
    n_copy.wait_send()
    for copy in beam_copies:
        copy.wait_send()
    for copy in copies.values():
        copy.wait_send()


def body(pulses, steering, merge_re, merge_im, range_shift, image_map):
    total, beams = pulses.shape[0], steering.shape[2]
    pulse_size, tile_size = lax.axis_size("pulse"), lax.axis_size("tile")
    pulse_bits, tile_bits = pulse_size.bit_length() - 1, tile_size.bit_length() - 1
    block_rows = total // (pulse_size * tile_size)
    columns = image_map.shape[4]
    width = 128
    chunks = 2 * columns // width
    steps = pulse_bits + tile_bits
    t = lax.axis_index("tile")
    bits = [t >> level & 1 for level in range(3)]

    def weight(level, source, target):
        take = lambda array: lax.dynamic_slice(
            array[level], (source * beams, target * beams), (beams, beams)
        )
        return take(merge_re), take(merge_im)

    steer = complex_block(steering[0], steering[1])
    w0 = jnp.concatenate(
        [complex_block(*weight(0, s, bits[0])) for s in (bits[0], 1 - bits[0])], axis=0
    )
    w1 = jnp.concatenate(
        [complex_block(*weight(1, bits[1], h)) for h in (bits[1], 1 - bits[1])], axis=1
    )
    w2 = jnp.stack([*weight(2, bits[2], bits[2]), *weight(2, bits[2], 1 - bits[2])])
    take = lambda level, source: lax.dynamic_index_in_dim(
        range_shift[level], source, 0, keepdims=False
    )
    table = jnp.stack(
        [
            jnp.tile(take(level, source), 4)
            for level, source in ((0, bits[0]), (0, 1 - bits[0]), (1, bits[1]), (2, bits[2]))
        ]
    ) + SHIFT
    vmem = pl.BlockSpec(memory_space=pltpu.VMEM)
    dma = pltpu.SemaphoreType.DMA
    padded = total + 2 * PAD
    return pl.pallas_call(
        functools.partial(kernel, pulse_bits, tile_bits, block_rows, width),
        out_shape=jax.ShapeDtypeStruct((block_rows, 2 * columns), F32),
        in_specs=[vmem] * 7,
        out_specs=vmem,
        scratch_shapes=[
            pltpu.VMEM((padded, 2 * beams), BF16),
            pltpu.VMEM((padded, 2 * beams), BF16),
            pltpu.VMEM((padded, 2 * beams), BF16),
            pltpu.VMEM((padded, 4 * beams), BF16),
            pltpu.VMEM((total, 4 * beams), BF16),
            pltpu.VMEM((2, beams, columns), BF16),
            pltpu.VMEM((2, beams, columns), BF16),
            pltpu.VMEM((2, beams, columns), BF16),
            pltpu.VMEM((4 * beams, 2 * columns), BF16),
            pltpu.VMEM((chunks, total // 2, width), F32),
            pltpu.VMEM((chunks, total, width), BF16),
            pltpu.VMEM((chunks, total, width), BF16),
            dma((4,)),
            dma((4,)),
            dma,
            dma,
            dma,
            dma,
            dma((steps, chunks)),
            dma((steps, chunks)),
        ],
        compiler_params=pltpu.CompilerParams(
            collective_id=0, has_side_effects=True, vmem_limit_bytes=60 * 2**20
        ),
    )(pulses.reshape(total, -1), steer, w0, w1, w2, image_map[0, 0], table)


def solution(mesh):
    placed = (
        P(None, None, ("pulse", "tile")),
        P(),
        P(),
        P(),
        P(),
        P("pulse", "tile", None, None, None),
    )
    return jax.shard_map(
        body, mesh=mesh, in_specs=placed, out_specs=P(("pulse", "tile"), None), check_vma=False
    )
```

```python
import functools

import jax
import jax.numpy as jnp
from jax import lax
from jax.experimental import pallas as pl
from jax.experimental.pallas import tpu as pltpu
from jax.sharding import PartitionSpec as P

SHIFT = 8
PAD = 16
STRIP = 128
MESH = pl.DeviceIdType.MESH
F32 = jnp.float32
BF16 = jnp.bfloat16


def bit_of(index, place):
    return index // 2**place % 2


def flip(index, place):
    return index + (1 - 2 * bit_of(index, place)) * 2**place


def orders(pulse_bits, tile_bits):
    pulse = [("pulse", place) for place in range(pulse_bits)]
    tile = [("tile", place) for place in range(1, tile_bits)]
    return [
        pulse + tile, pulse[::-1] + tile, tile + pulse,
        pulse + tile, pulse[::-1] + tile, tile + pulse[::-1],
        pulse + tile, pulse[::-1] + tile,
    ]


def shifted(ref, start, rows, table):
    columns = []
    for column in range(0, ref.shape[1], 128):
        shift = table[:, column : column + 128]
        masks = [(shift & step) != 0 for step in (1, 2, 4, 8, 16)]
        strips = []
        for strip in range(0, rows, STRIP):
            piece = ref[pl.ds(start + strip, STRIP + 2 * PAD), column : column + 128]
            piece = piece.astype(F32)[PAD - SHIFT :]
            held = piece.shape[0]
            for mask, step in zip(masks, (1, 2, 4)):
                piece = jnp.where(mask, pltpu.roll(piece, held - step, 0), piece)
            piece = jnp.where(masks[3], piece[8 : STRIP + 24], piece[: STRIP + 16])
            piece = jnp.where(masks[4], piece[16 : STRIP + 16], piece[:STRIP])
            strips.append(piece.astype(BF16))
        columns.append(jnp.concatenate(strips, axis=0))
    return jnp.concatenate(columns, axis=1)


def kernel(
    pulse_bits, tile_bits, block_rows, width,
    rows_ref, steer_ref, re_ref, im_ref, shift_ref, map_ref, out_ref,
    real, imag, w0_ref, w1_ref, w2_ref, b0, bp, b1, b2, b3, map_in, own, other, final, acc, send, recv,
    beam_s, beam_r, map_s, map_r, n_s, n_r, sum_s, sum_r,
):
    p, t = lax.axis_index("pulse"), lax.axis_index("tile")
    where = {"pulse": p, "tile": t}
    total = rows_ref.shape[0] // 2
    beams = map_ref.shape[1]
    columns = map_ref.shape[2]
    pieces = columns // width
    chunks = 2 * pieces
    streams = orders(pulse_bits, tile_bits)
    steps = pulse_bits + tile_bits
    tile = 512
    bits = [bit_of(t, level) for level in range(3)]

    def device(axis, place):
        found = dict(where)
        found[axis] = flip(where[axis], place)
        return (found["pulse"], found["tile"])

    partners = [("pulse", place) for place in range(pulse_bits)]
    partners += [("tile", place) for place in range(tile_bits)]
    barrier = pltpu.get_barrier_semaphore()
    for axis, place in partners:
        pl.semaphore_signal(barrier, inc=1, device_id=device(axis, place), device_id_type=MESH)

    def product(left, right):
        return jnp.dot(left, right, preferred_element_type=F32)

    part = total // 4

    def steer(piece):
        @pl.loop(0, part // tile)
        def _(i):
            start = pl.multiple_of(piece * part + i * tile, tile)
            both = rows_ref[pl.ds(2 * start, 2 * tile), :]
            real[...] = product(both, steer_ref[0])
            imag[...] = product(both, steer_ref[1])
            even, odd = pl.ds(0, tile, stride=2), pl.ds(1, tile, stride=2)
            to = pl.ds(start + PAD, tile)
            b0[to, :beams] = (real[even, :] - imag[odd, :]).astype(BF16)
            b0[to, beams:] = (imag[even, :] + real[odd, :]).astype(BF16)

    for ref in (b0, bp, b1, b2):
        edge = jnp.zeros((PAD, ref.shape[1]), BF16)
        ref[0:PAD, :] = edge
        ref[PAD + total : 2 * PAD + total, :] = edge
    steer(0)
    pl.semaphore_wait(barrier, len(partners))

    def span_of(piece):
        return slice(piece * width, (piece + 1) * width)

    map_copies = [
        pltpu.make_async_remote_copy(
            src_ref=map_ref.at[:, :, span_of(piece)], dst_ref=map_in.at[:, :, span_of(piece)],
            send_sem=map_s.at[piece], recv_sem=map_r.at[piece],
            device_id=device("tile", 2), device_id_type=MESH,
        )
        for piece in range(pieces)
    ]
    n_copies = [
        pltpu.make_async_remote_copy(
            src_ref=own.at[:, :, span_of(piece)], dst_ref=other.at[:, :, span_of(piece)],
            send_sem=n_s.at[piece], recv_sem=n_r.at[piece],
            device_id=device("tile", 1), device_id_type=MESH,
        )
        for piece in range(pieces)
    ]
    beam_copies = [
        pltpu.make_async_remote_copy(
            src_ref=b0.at[pl.ds(PAD + piece * part, part), :],
            dst_ref=bp.at[pl.ds(PAD + piece * part, part), :],
            send_sem=beam_s.at[piece], recv_sem=beam_r.at[piece],
            device_id=device("tile", 0), device_id_type=MESH,
        )
        for piece in range(4)
    ]
    for copy in map_copies:
        copy.start()
    beam_copies[0].start()
    for piece in range(1, 4):
        steer(piece)
        beam_copies[piece].start()

    def weight(level, source, target):
        at = (level, pl.ds(pl.multiple_of(source * beams, beams), beams))
        at += (pl.ds(pl.multiple_of(target * beams, beams), beams),)
        return re_ref[at], im_ref[at]

    def put_block(ref, row, column, parts):
        ref[row : row + beams, column : column + beams] = parts[0]
        ref[row : row + beams, column + beams : column + 2 * beams] = parts[1]
        ref[row + beams : row + 2 * beams, column : column + beams] = -parts[1]
        ref[row + beams : row + 2 * beams, column + beams : column + 2 * beams] = parts[0]

    def offsets(level, source):
        line = jnp.where(source == 0, shift_ref[level, 0:1, :], shift_ref[level, 1:2, :])
        return jnp.concatenate([line, line], axis=1) + SHIFT

    for at, flipped in ((0, bits[0]), (2 * beams, 1 - bits[0])):
        put_block(w0_ref, at, 0, weight(0, flipped, bits[0]))
    for at, flipped in ((0, bits[1]), (2 * beams, 1 - bits[1])):
        put_block(w1_ref, 0, at, weight(1, bits[1], flipped))
    for at, flipped in ((0, bits[2]), (2, 1 - bits[2])):
        w2_ref[at], w2_ref[at + 1] = weight(2, bits[2], flipped)

    tables = [offsets(0, bits[0]), offsets(0, 1 - bits[0]), offsets(1, bits[1]), offsets(2, bits[2])]

    def level_0(low, high):
        @pl.loop(low, high)
        def _(i):
            start = pl.multiple_of(i * tile, tile)
            mine = shifted(b0, start, tile, tables[0])
            theirs = shifted(bp, start, tile, tables[1])
            merged = product(mine, w0_ref[: 2 * beams, :])
            merged += product(theirs, w0_ref[2 * beams :, :])
            b1[pl.ds(start + PAD, tile), :] = merged.astype(BF16)

    done = 0
    for piece in range(4):
        beam_copies[piece].wait_recv()
        reach = total // tile if piece == 3 else (piece + 1) * part // tile - 1
        level_0(done, reach)
        done = reach

    def compose(piece):
        span = span_of(piece)
        map_copies[piece].wait_recv()
        left = [w2_ref[i] for i in range(4)]
        right = [map_ref[0, :, span], map_ref[1, :, span], map_in[0, :, span], map_in[1, :, span]]
        own[0, :, span] = (
            product(left[0], right[0]) - product(left[1], right[1])
            + product(left[2], right[2]) - product(left[3], right[3])
        ).astype(BF16)
        own[1, :, span] = (
            product(left[0], right[1]) + product(left[1], right[0])
            + product(left[2], right[3]) + product(left[3], right[2])
        ).astype(BF16)
        n_copies[piece].start()

    for piece in range(pieces // 2):
        compose(piece)

    @pl.loop(0, total // tile)
    def _(i):
        start = pl.multiple_of(i * tile, tile)
        mine = shifted(b1, start, tile, tables[2])
        b2[pl.ds(start + PAD, tile), :] = product(mine, w1_ref[...]).astype(BF16)

    for piece in range(pieces // 2, pieces):
        compose(piece)

    twice = jnp.concatenate([tables[3], tables[3]], axis=1)

    @pl.loop(0, total // tile)
    def _(i):
        start = pl.multiple_of(i * tile, tile)
        b3[pl.ds(start, tile), :] = shifted(b2, start, tile, twice)

    core = bit_of(t, 0)
    half = total // 2
    bases = [total - (total >> step) for step in range(steps)]
    copies = {}

    def launch(step, chunk, axis, place):
        span = pl.ds(bases[step], half >> step)
        copies[step, chunk] = copy = pltpu.make_async_remote_copy(
            src_ref=send.at[chunk, span, :], dst_ref=recv.at[chunk, span, :],
            send_sem=sum_s.at[step, chunk], recv_sem=sum_r.at[step, chunk],
            device_id=device(axis, place), device_id_type=MESH,
        )
        copy.start()

    def form(piece):
        span = span_of(piece)
        n_copies[piece].wait_recv()
        for at, source in ((0, own), (2 * beams, other)):
            put_block(final, at, 0, (source[0, :, span], source[1, :, span]))
        chunk_set = (2 * piece, 2 * piece + 1)

        @pl.loop(0, total // tile)
        def _(i):
            start = pl.multiple_of(i * tile, tile)
            value = product(b3[pl.ds(start, tile), :], final[...])
            for pair in range(tile // (2 * block_rows)):
                low = value[2 * pair * block_rows : (2 * pair + 1) * block_rows]
                high = value[(2 * pair + 1) * block_rows : (2 * pair + 2) * block_rows]
                keep = jnp.where(core == 0, low, high)
                leave = jnp.where(core == 0, high, low).astype(BF16)
                number = i * (tile // (2 * block_rows)) + pair
                for at, chunk in enumerate(chunk_set):
                    order = streams[chunk % len(streams)]
                    index = 0
                    for axis, place in order:
                        where_bit = place - 1 if axis == "tile" else place + tile_bits - 1
                        index = index * 2 + bit_of(number, where_bit)
                    span = pl.ds(pl.multiple_of(index * block_rows, block_rows), block_rows)
                    acc[chunk, span, :] = keep[:, at * width : (at + 1) * width]
                    send[chunk, span, :] = leave[:, at * width : (at + 1) * width]

        for chunk in chunk_set:
            launch(0, chunk, "tile", 0)

    bases_live = {chunk: 0 for chunk in range(chunks)}

    def fold(step, chunk):
        copies[step, chunk].wait_recv()
        rows = half >> step
        live = bases_live[chunk]
        if step == steps - 1:
            span = pl.ds(pl.multiple_of(live, rows), rows)
            got = recv[chunk, pl.ds(bases[step], rows), :].astype(F32)
            first = chunk % 2 * columns + chunk // 2 * width
            out_ref[:, first : first + width] = acc[chunk, span, :] + got
            return
        axis, place = streams[chunk % len(streams)][step]
        rest = rows // 2
        kept = bit_of(where[axis], place)
        size = min(rest, 256)

        @pl.loop(0, rest // size)
        def _(i):
            at = (1 - kept) * rest + i * size
            value = acc[chunk, pl.ds(pl.multiple_of(live + at, size), size), :]
            value += recv[chunk, pl.ds(pl.multiple_of(bases[step] + at, size), size), :].astype(F32)
            to = pl.ds(pl.multiple_of(bases[step + 1] + i * size, size), size)
            send[chunk, to, :] = value.astype(BF16)

        launch(step + 1, chunk, axis, place)

        @pl.loop(0, rest // size)
        def _(i):
            at = kept * rest + i * size
            span = pl.ds(pl.multiple_of(live + at, size), size)
            got = recv[chunk, pl.ds(pl.multiple_of(bases[step] + at, size), size), :]
            acc[chunk, span, :] += got.astype(F32)

        bases_live[chunk] = live + kept * rest

    for piece in range(pieces):
        form(piece)
        if piece > 0:
            fold(0, 2 * piece - 2)
            fold(0, 2 * piece - 1)
    fold(0, chunks - 2)
    fold(0, chunks - 1)
    for step in range(1, steps):
        for chunk in range(chunks):
            fold(step, chunk)

    for copy in (*map_copies, *n_copies, *beam_copies, *copies.values()):
        copy.wait_send()


def body(pulses, steering, merge_re, merge_im, range_shift, image_map):
    total, beams = pulses.shape[0], steering.shape[2]
    pulse_size, tile_size = lax.axis_size("pulse"), lax.axis_size("tile")
    pulse_bits, tile_bits = pulse_size.bit_length() - 1, tile_size.bit_length() - 1
    block_rows = total // (pulse_size * tile_size)
    columns = image_map.shape[4]
    width = 128
    chunks = 2 * columns // width
    steps = pulse_bits + tile_bits
    vmem = pl.BlockSpec(memory_space=pltpu.VMEM)
    dma = pltpu.SemaphoreType.DMA
    padded = total + 2 * PAD
    return pl.pallas_call(
        functools.partial(kernel, pulse_bits, tile_bits, block_rows, width),
        out_shape=jax.ShapeDtypeStruct((block_rows, 2 * columns), F32),
        in_specs=[vmem] * 6,
        out_specs=vmem,
        scratch_shapes=[
            pltpu.VMEM((1024, beams), F32),
            pltpu.VMEM((1024, beams), F32),
            pltpu.VMEM((4 * beams, 2 * beams), BF16),
            pltpu.VMEM((2 * beams, 4 * beams), BF16),
            pltpu.VMEM((4, beams, beams), BF16),
            pltpu.VMEM((padded, 2 * beams), BF16),
            pltpu.VMEM((padded, 2 * beams), BF16),
            pltpu.VMEM((padded, 2 * beams), BF16),
            pltpu.VMEM((padded, 4 * beams), BF16),
            pltpu.VMEM((total, 4 * beams), BF16),
            pltpu.VMEM((2, beams, columns), BF16),
            pltpu.VMEM((2, beams, columns), BF16),
            pltpu.VMEM((2, beams, columns), BF16),
            pltpu.VMEM((4 * beams, 2 * width), BF16),
            pltpu.VMEM((chunks, total // 2, width), F32),
            pltpu.VMEM((chunks, total, width), BF16),
            pltpu.VMEM((chunks, total, width), BF16),
            dma((4,)),
            dma((4,)),
            dma((chunks // 2,)),
            dma((chunks // 2,)),
            dma((chunks // 2,)),
            dma((chunks // 2,)),
            dma((steps, chunks)),
            dma((steps, chunks)),
        ],
        compiler_params=pltpu.CompilerParams(
            collective_id=0, has_side_effects=True, vmem_limit_bytes=60 * 2**20
        ),
    )(pulses.reshape(2 * total, -1), steering, merge_re, merge_im, range_shift, image_map[0, 0])


def solution(mesh):
    placed = (
        P(None, None, ("pulse", "tile")),
        P(),
        P(),
        P(),
        P(),
        P("pulse", "tile", None, None, None),
    )
    return jax.shard_map(
        body, mesh=mesh, in_specs=placed, out_specs=P(("pulse", "tile"), None), check_vma=False
    )
```

```python
import functools

import jax
import jax.numpy as jnp
from jax import lax
from jax.experimental import pallas as pl
from jax.experimental.pallas import tpu as pltpu
from jax.sharding import PartitionSpec as P

SHIFT = 8
PAD = 16
STRIP = 128
MESH = pl.DeviceIdType.MESH
F32 = jnp.float32
BF16 = jnp.bfloat16


def bit_of(index, place):
    return index // 2**place % 2


def flip(index, place):
    return index + (1 - 2 * bit_of(index, place)) * 2**place


def orders(pulse_bits, tile_bits):
    pulse = [("pulse", place) for place in range(pulse_bits)]
    tile = [("tile", place) for place in range(1, tile_bits)]
    return [
        pulse + tile, pulse[::-1] + tile, tile + pulse,
        pulse + tile, pulse[::-1] + tile, tile + pulse[::-1],
        pulse + tile, pulse[::-1] + tile,
    ]


def shifted(ref, start, rows, table):
    columns = []
    lane_rows = lax.broadcasted_iota(jnp.int32, (8, 128), 0)
    for column in range(0, ref.shape[1], 128):
        shift = jnp.broadcast_to(table[:, column : column + 128], (8, 128))
        moved = lane_rows + (shift & 7)
        index, wraps = moved & 7, moved >= 8
        first, second = shift < 8, shift < 16
        strips = []
        for strip in range(0, rows, STRIP):
            piece = ref[pl.ds(start + strip, STRIP + 2 * PAD), column : column + 128]
            piece = piece.astype(F32)
            turned = [
                jnp.take_along_axis(piece[at : at + 8], index, axis=0, mode="promise_in_bounds")
                for at in range(PAD - SHIFT, STRIP + 2 * PAD, 8)
            ]
            joined = [jnp.where(wraps, b, a) for a, b in zip(turned, turned[1:])]
            picked = [
                jnp.where(first, a, jnp.where(second, b, c))
                for a, b, c in zip(joined, joined[1:], joined[2:])
            ]
            strips.append(jnp.concatenate(picked, axis=0).astype(BF16))
        columns.append(jnp.concatenate(strips, axis=0))
    return jnp.concatenate(columns, axis=1)


def kernel(
    pulse_bits, tile_bits, block_rows, width,
    rows_ref, steer_ref, re_ref, im_ref, shift_ref, map_ref, out_ref,
    real, imag, w0_ref, w1_ref, w2_ref, b0, bp, b1, b2, b3, map_in, own, other, final, acc, send, recv,
    beam_s, beam_r, map_s, map_r, n_s, n_r, sum_s, sum_r,
):
    p, t = lax.axis_index("pulse"), lax.axis_index("tile")
    where = {"pulse": p, "tile": t}
    total = rows_ref.shape[0] // 2
    beams = map_ref.shape[1]
    columns = map_ref.shape[2]
    pieces = columns // width
    chunks = 2 * pieces
    streams = orders(pulse_bits, tile_bits)
    steps = pulse_bits + tile_bits
    tile = 512
    bits = [bit_of(t, level) for level in range(3)]

    def device(axis, place):
        found = dict(where)
        found[axis] = flip(where[axis], place)
        return (found["pulse"], found["tile"])

    partners = [("pulse", place) for place in range(pulse_bits)]
    partners += [("tile", place) for place in range(tile_bits)]
    barrier = pltpu.get_barrier_semaphore()
    for axis, place in partners:
        pl.semaphore_signal(barrier, inc=1, device_id=device(axis, place), device_id_type=MESH)

    def product(left, right):
        return jnp.dot(left, right, preferred_element_type=F32)

    part = total // 4

    def steer(piece):
        @pl.loop(0, part // tile)
        def _(i):
            start = pl.multiple_of(piece * part + i * tile, tile)
            both = rows_ref[pl.ds(2 * start, 2 * tile), :]
            real[...] = product(both, steer_ref[0])
            imag[...] = product(both, steer_ref[1])
            even, odd = pl.ds(0, tile, stride=2), pl.ds(1, tile, stride=2)
            to = pl.ds(start + PAD, tile)
            b0[to, :beams] = (real[even, :] - imag[odd, :]).astype(BF16)
            b0[to, beams:] = (imag[even, :] + real[odd, :]).astype(BF16)

    for ref in (b0, bp, b1, b2):
        edge = jnp.zeros((PAD, ref.shape[1]), BF16)
        ref[0:PAD, :] = edge
        ref[PAD + total : 2 * PAD + total, :] = edge
    steer(0)
    pl.semaphore_wait(barrier, len(partners))

    def span_of(piece):
        return slice(piece * width, (piece + 1) * width)

    map_copies = [
        pltpu.make_async_remote_copy(
            src_ref=map_ref.at[:, :, span_of(piece)], dst_ref=map_in.at[:, :, span_of(piece)],
            send_sem=map_s.at[piece], recv_sem=map_r.at[piece],
            device_id=device("tile", 2), device_id_type=MESH,
        )
        for piece in range(pieces)
    ]
    n_copies = [
        pltpu.make_async_remote_copy(
            src_ref=own.at[:, :, span_of(piece)], dst_ref=other.at[:, :, span_of(piece)],
            send_sem=n_s.at[piece], recv_sem=n_r.at[piece],
            device_id=device("tile", 1), device_id_type=MESH,
        )
        for piece in range(pieces)
    ]
    beam_copies = [
        pltpu.make_async_remote_copy(
            src_ref=b0.at[pl.ds(PAD + piece * part, part), :],
            dst_ref=bp.at[pl.ds(PAD + piece * part, part), :],
            send_sem=beam_s.at[piece], recv_sem=beam_r.at[piece],
            device_id=device("tile", 0), device_id_type=MESH,
        )
        for piece in range(4)
    ]
    for copy in map_copies:
        copy.start()
    beam_copies[0].start()
    for piece in range(1, 4):
        steer(piece)
        beam_copies[piece].start()

    def weight(level, source, target):
        at = (level, pl.ds(pl.multiple_of(source * beams, beams), beams))
        at += (pl.ds(pl.multiple_of(target * beams, beams), beams),)
        return re_ref[at], im_ref[at]

    def put_block(ref, row, column, parts):
        ref[row : row + beams, column : column + beams] = parts[0]
        ref[row : row + beams, column + beams : column + 2 * beams] = parts[1]
        ref[row + beams : row + 2 * beams, column : column + beams] = -parts[1]
        ref[row + beams : row + 2 * beams, column + beams : column + 2 * beams] = parts[0]

    def offsets(level, source):
        line = jnp.where(source == 0, shift_ref[level, 0:1, :], shift_ref[level, 1:2, :])
        return jnp.concatenate([line, line], axis=1) + SHIFT

    for at, flipped in ((0, bits[0]), (2 * beams, 1 - bits[0])):
        put_block(w0_ref, at, 0, weight(0, flipped, bits[0]))
    for at, flipped in ((0, bits[1]), (2 * beams, 1 - bits[1])):
        put_block(w1_ref, 0, at, weight(1, bits[1], flipped))
    for at, flipped in ((0, bits[2]), (2, 1 - bits[2])):
        w2_ref[at], w2_ref[at + 1] = weight(2, bits[2], flipped)

    tables = [offsets(0, bits[0]), offsets(0, 1 - bits[0]), offsets(1, bits[1]), offsets(2, bits[2])]

    def level_0(low, high):
        @pl.loop(low, high)
        def _(i):
            start = pl.multiple_of(i * tile, tile)
            mine = shifted(b0, start, tile, tables[0])
            theirs = shifted(bp, start, tile, tables[1])
            merged = product(mine, w0_ref[: 2 * beams, :])
            merged += product(theirs, w0_ref[2 * beams :, :])
            b1[pl.ds(start + PAD, tile), :] = merged.astype(BF16)

    done = 0
    for piece in range(4):
        beam_copies[piece].wait_recv()
        reach = total // tile if piece == 3 else (piece + 1) * part // tile - 1
        level_0(done, reach)
        done = reach

    def compose(piece):
        span = span_of(piece)
        map_copies[piece].wait_recv()
        left = [w2_ref[i] for i in range(4)]
        right = [map_ref[0, :, span], map_ref[1, :, span], map_in[0, :, span], map_in[1, :, span]]
        own[0, :, span] = (
            product(left[0], right[0]) - product(left[1], right[1])
            + product(left[2], right[2]) - product(left[3], right[3])
        ).astype(BF16)
        own[1, :, span] = (
            product(left[0], right[1]) + product(left[1], right[0])
            + product(left[2], right[3]) + product(left[3], right[2])
        ).astype(BF16)
        n_copies[piece].start()

    for piece in range(pieces // 2):
        compose(piece)

    @pl.loop(0, total // tile)
    def _(i):
        start = pl.multiple_of(i * tile, tile)
        mine = shifted(b1, start, tile, tables[2])
        b2[pl.ds(start + PAD, tile), :] = product(mine, w1_ref[...]).astype(BF16)

    for piece in range(pieces // 2, pieces):
        compose(piece)

    twice = jnp.concatenate([tables[3], tables[3]], axis=1)

    @pl.loop(0, total // tile)
    def _(i):
        start = pl.multiple_of(i * tile, tile)
        b3[pl.ds(start, tile), :] = shifted(b2, start, tile, twice)

    core = bit_of(t, 0)
    half = total // 2
    bases = [total - (total >> step) for step in range(steps)]
    copies = {}

    def launch(step, chunk, axis, place):
        span = pl.ds(bases[step], half >> step)
        copies[step, chunk] = copy = pltpu.make_async_remote_copy(
            src_ref=send.at[chunk, span, :], dst_ref=recv.at[chunk, span, :],
            send_sem=sum_s.at[step, chunk], recv_sem=sum_r.at[step, chunk],
            device_id=device(axis, place), device_id_type=MESH,
        )
        copy.start()

    def form(piece):
        span = span_of(piece)
        n_copies[piece].wait_recv()
        for at, source in ((0, own), (2 * beams, other)):
            put_block(final, at, 0, (source[0, :, span], source[1, :, span]))
        chunk_set = (2 * piece, 2 * piece + 1)

        @pl.loop(0, total // tile)
        def _(i):
            start = pl.multiple_of(i * tile, tile)
            value = product(b3[pl.ds(start, tile), :], final[...])
            for pair in range(tile // (2 * block_rows)):
                low = value[2 * pair * block_rows : (2 * pair + 1) * block_rows]
                high = value[(2 * pair + 1) * block_rows : (2 * pair + 2) * block_rows]
                keep = jnp.where(core == 0, low, high)
                leave = jnp.where(core == 0, high, low).astype(BF16)
                number = i * (tile // (2 * block_rows)) + pair
                for at, chunk in enumerate(chunk_set):
                    order = streams[chunk % len(streams)]
                    index = 0
                    for axis, place in order:
                        where_bit = place - 1 if axis == "tile" else place + tile_bits - 1
                        index = index * 2 + bit_of(number, where_bit)
                    span = pl.ds(pl.multiple_of(index * block_rows, block_rows), block_rows)
                    acc[chunk, span, :] = keep[:, at * width : (at + 1) * width]
                    send[chunk, span, :] = leave[:, at * width : (at + 1) * width]

        for chunk in chunk_set:
            launch(0, chunk, "tile", 0)

    bases_live = {chunk: 0 for chunk in range(chunks)}

    def fold(step, chunk):
        copies[step, chunk].wait_recv()
        rows = half >> step
        live = bases_live[chunk]
        if step == steps - 1:
            span = pl.ds(pl.multiple_of(live, rows), rows)
            got = recv[chunk, pl.ds(bases[step], rows), :].astype(F32)
            first = chunk % 2 * columns + chunk // 2 * width
            out_ref[:, first : first + width] = acc[chunk, span, :] + got
            return
        axis, place = streams[chunk % len(streams)][step]
        rest = rows // 2
        kept = bit_of(where[axis], place)
        size = min(rest, 256)

        @pl.loop(0, rest // size)
        def _(i):
            at = (1 - kept) * rest + i * size
            value = acc[chunk, pl.ds(pl.multiple_of(live + at, size), size), :]
            value += recv[chunk, pl.ds(pl.multiple_of(bases[step] + at, size), size), :].astype(F32)
            to = pl.ds(pl.multiple_of(bases[step + 1] + i * size, size), size)
            send[chunk, to, :] = value.astype(BF16)

        launch(step + 1, chunk, axis, place)

        @pl.loop(0, rest // size)
        def _(i):
            at = kept * rest + i * size
            span = pl.ds(pl.multiple_of(live + at, size), size)
            got = recv[chunk, pl.ds(pl.multiple_of(bases[step] + at, size), size), :]
            acc[chunk, span, :] += got.astype(F32)

        bases_live[chunk] = live + kept * rest

    for piece in range(pieces):
        form(piece)
        if piece > 0:
            fold(0, 2 * piece - 2)
            fold(0, 2 * piece - 1)
    fold(0, chunks - 2)
    fold(0, chunks - 1)
    for step in range(1, steps):
        for chunk in range(chunks):
            fold(step, chunk)

    for copy in (*map_copies, *n_copies, *beam_copies, *copies.values()):
        copy.wait_send()


def body(pulses, steering, merge_re, merge_im, range_shift, image_map):
    total, beams = pulses.shape[0], steering.shape[2]
    pulse_size, tile_size = lax.axis_size("pulse"), lax.axis_size("tile")
    pulse_bits, tile_bits = pulse_size.bit_length() - 1, tile_size.bit_length() - 1
    block_rows = total // (pulse_size * tile_size)
    columns = image_map.shape[4]
    width = 128
    chunks = 2 * columns // width
    steps = pulse_bits + tile_bits
    vmem = pl.BlockSpec(memory_space=pltpu.VMEM)
    dma = pltpu.SemaphoreType.DMA
    padded = total + 2 * PAD
    return pl.pallas_call(
        functools.partial(kernel, pulse_bits, tile_bits, block_rows, width),
        out_shape=jax.ShapeDtypeStruct((block_rows, 2 * columns), F32),
        in_specs=[vmem] * 6,
        out_specs=vmem,
        scratch_shapes=[
            pltpu.VMEM((1024, beams), F32),
            pltpu.VMEM((1024, beams), F32),
            pltpu.VMEM((4 * beams, 2 * beams), BF16),
            pltpu.VMEM((2 * beams, 4 * beams), BF16),
            pltpu.VMEM((4, beams, beams), BF16),
            pltpu.VMEM((padded, 2 * beams), BF16),
            pltpu.VMEM((padded, 2 * beams), BF16),
            pltpu.VMEM((padded, 2 * beams), BF16),
            pltpu.VMEM((padded, 4 * beams), BF16),
            pltpu.VMEM((total, 4 * beams), BF16),
            pltpu.VMEM((2, beams, columns), BF16),
            pltpu.VMEM((2, beams, columns), BF16),
            pltpu.VMEM((2, beams, columns), BF16),
            pltpu.VMEM((4 * beams, 2 * width), BF16),
            pltpu.VMEM((chunks, total // 2, width), F32),
            pltpu.VMEM((chunks, total, width), BF16),
            pltpu.VMEM((chunks, total, width), BF16),
            dma((4,)),
            dma((4,)),
            dma((chunks // 2,)),
            dma((chunks // 2,)),
            dma((chunks // 2,)),
            dma((chunks // 2,)),
            dma((steps, chunks)),
            dma((steps, chunks)),
        ],
        compiler_params=pltpu.CompilerParams(
            collective_id=0, has_side_effects=True, vmem_limit_bytes=60 * 2**20
        ),
    )(pulses.reshape(2 * total, -1), steering, merge_re, merge_im, range_shift, image_map[0, 0])


def solution(mesh):
    placed = (
        P(None, None, ("pulse", "tile")),
        P(),
        P(),
        P(),
        P(),
        P("pulse", "tile", None, None, None),
    )
    return jax.shard_map(
        body, mesh=mesh, in_specs=placed, out_specs=P(("pulse", "tile"), None), check_vma=False
    )
```
